32 devices in a mesh: row: 4 (over y, core), col: 8 (over z, x).
Axes of the slice: x: 2, y: 2, z: 4, core: 2. Of those that a mesh axis runs over, the one named last changes fastest.
Arguments:
- tokens: bfloat16 [40, 8192], P('col', 'row'), may hold values from -6 to 6
- grad_out: bfloat16 [40, 8192], P('col', 'row'), may hold values from -6 to 6
- gate_weight: bfloat16 [8192, 28672], P('row', 'col'), may hold values from -0.0625 to 0.0625
- up_weight: bfloat16 [8192, 28672], P('row', 'col'), may hold values from -0.0625 to 0.0625
- down_weight: bfloat16 [28672, 8192], P('col', 'row'), may hold values from -0.03125 to 0.03125
Outputs:
- grad_tokens: bfloat16 [40, 8192], P('col', 'row')
- grad_gate_weight: bfloat16 [8192, 28672], P('row', 'col')
- grad_up_weight: bfloat16 [8192, 28672], P('row', 'col')
- grad_down_weight: bfloat16 [28672, 8192], P('col', 'row')
The draws below stay inside these ranges and needn't reach their ends.
All inputs are finite; a program needn't handle non-finite values.
Results may differ from the reference program's by a relative error of at most 0.0049.
Values may be sent and summed in bfloat16 or wider, within the bound.
A program may use at most 192 MiB of HBM per device.

```python
import jax
import jax.numpy as jnp

D = 8192
FF = 28672
TOKENS = 40


def steps_of(stream_key, dims, shards, low, top_value):
    def one(axis_at, blocks):
        steps = jax.random.uniform(jax.random.fold_in(jax.random.fold_in(stream_key, 6), axis_at), (blocks,), jnp.float32, low / len(shards), top_value / len(shards))
        return jnp.repeat(jnp.exp(steps), dims[axis_at] // blocks).reshape((-1,) + (1,) * (len(dims) - axis_at - 1))

    factor_of = one(*shards[0])
    for cut in shards[1:]:
        factor_of = factor_of * one(*cut)
    return factor_of


def gaussian(key, shape, spread, reach, pieces=(), dtype=jnp.bfloat16):
    gain = steps_of(key, shape, pieces, -0.22, 0.18) if pieces else 1.0
    array = jax.random.normal(key, shape, jnp.float32) * spread * gain
    return jnp.minimum(jnp.maximum(array, -reach), reach).astype(dtype)


def setup_inputs(seed: int = 0) -> dict:
    seeds = jax.random.split(jax.random.key(seed), 6)
    tokens = gaussian(seeds[0], (TOKENS, D), 1.0, 6.0, ((0, 8), (1, 4)))
    grad_out = gaussian(seeds[1], (TOKENS, D), 1.0, 6.0, ((0, 8), (1, 4)))
    gate_weight = gaussian(seeds[2], (D, FF), D ** -0.5, 0.0625, ((0, 4), (1, 8)))
    up_weight = gaussian(seeds[3], (D, FF), D ** -0.5, 0.0625, ((0, 4), (1, 8)))
    down_weight = gaussian(seeds[4], (FF, D), FF ** -0.5, 0.03125, ((0, 8), (1, 4)))
    return dict(tokens=tokens, grad_out=grad_out, gate_weight=gate_weight, up_weight=up_weight, down_weight=down_weight)


def hidden_grads(gate_sum, up_sum, back_sum):
    sigmoid_gate = 1.0 / (1.0 + jnp.exp(-gate_sum))
    activated = gate_sum * sigmoid_gate
    hidden = (activated * up_sum).astype(jnp.bfloat16)
    grad_up = (back_sum * activated).astype(jnp.bfloat16)
    slope = sigmoid_gate * (1.0 + gate_sum * (1.0 - sigmoid_gate))
    grad_gate = (back_sum * up_sum * slope).astype(jnp.bfloat16)
    return hidden, grad_gate, grad_up


def reference(tokens, grad_out, gate_weight, up_weight, down_weight):
    gate_sum = jnp.dot(tokens, gate_weight, preferred_element_type=jnp.float32)
    up_sum = jnp.dot(tokens, up_weight, preferred_element_type=jnp.float32)
    back_sum = jnp.dot(grad_out, down_weight.T, preferred_element_type=jnp.float32)
    hidden, grad_gate, grad_up = hidden_grads(gate_sum, up_sum, back_sum)
    grad_down_weight = jnp.dot(hidden.T, grad_out, preferred_element_type=jnp.float32).astype(jnp.bfloat16)
    grad_gate_weight = jnp.dot(tokens.T, grad_gate, preferred_element_type=jnp.float32).astype(jnp.bfloat16)
    grad_up_weight = jnp.dot(tokens.T, grad_up, preferred_element_type=jnp.float32).astype(jnp.bfloat16)
    grad_tokens = jnp.dot(grad_gate, gate_weight.T, preferred_element_type=jnp.float32)
    grad_tokens = grad_tokens + jnp.dot(grad_up, up_weight.T, preferred_element_type=jnp.float32)
    return grad_tokens.astype(jnp.bfloat16), grad_gate_weight, grad_up_weight, grad_down_weight
```

```python
import functools

import jax
import jax.numpy as jnp
from jax import lax
from jax.experimental import pallas as pl
from jax.experimental.pallas import tpu as pltpu
from jax.sharding import PartitionSpec as P

F32 = jnp.float32
BF16 = jnp.bfloat16
LAST = (((1,), (1,)), ((), ()))
MESH = pl.DeviceIdType.MESH


def hidden_grads(gate_sum, up_sum, back_sum):
    sigmoid_gate = 1.0 / (1.0 + jnp.exp(-gate_sum))
    activated = gate_sum * sigmoid_gate
    hidden = (activated * up_sum).astype(BF16)
    grad_up = (back_sum * activated).astype(BF16)
    slope = sigmoid_gate * (1.0 + gate_sum * (1.0 - sigmoid_gate))
    grad_gate = (back_sum * up_sum * slope).astype(BF16)
    return (hidden, grad_gate, grad_up)


def exchange_kernel(
    rows, cols, tok_in, grad_in, gate_hbm, up_hbm, down_hbm,
    tok_out, grad_out, acts_out, dtok_out,
    gate_buf, up_buf, down_buf, tok_slots, grad_slots, stage, tok_all, grad_all,
    part_send, part_recv, acts, acc, dtok_send, dtok_recv,
    load_sem, own_sem, tok_ssem, tok_rsem, part_ssem, part_rsem,
    acts_ssem, acts_rsem, fwd_ssem, fwd_rsem, dtok_ssem, dtok_rsem, out_sem,
):
    row, col = lax.axis_index("row"), lax.axis_index("col")
    chips = rows // 2
    chip, core = row // 2, row % 2
    width = gate_buf.shape[2]
    few = tok_in.shape[0]

    def peer(dy, dc):
        return ((chip + dy) % chips) * 2 + (core + dc) % 2

    offsets = [(dy, dc) for dy in range(1, chips) for dc in (0, 1)] + [(0, 1), (0, 0)]

    loads = []
    for o, (dy, dc) in enumerate(offsets):
        at = pl.multiple_of(peer(dy, dc) * width, 128)
        trio = (
            pltpu.make_async_copy(gate_hbm.at[:, pl.ds(at, width)], gate_buf.at[o], load_sem.at[0, o]),
            pltpu.make_async_copy(up_hbm.at[:, pl.ds(at, width)], up_buf.at[o], load_sem.at[1, o]),
            pltpu.make_async_copy(down_hbm.at[pl.ds(at, width), :], down_buf.at[o], load_sem.at[2, o]),
        )
        loads.append(trio)
    for load in loads[0]:
        load.start()

    barrier = pltpu.get_barrier_semaphore()
    for dy, dc in offsets[:-1]:
        pl.semaphore_signal(barrier, inc=1, device_id=(peer(dy, dc), col), device_id_type=MESH)
    for s in range(1, cols):
        pl.semaphore_signal(barrier, inc=1, device_id=(row, (col + s) % cols), device_id_type=MESH)
    own_tok = pltpu.make_async_copy(tok_in, tok_slots.at[col], own_sem.at[0])
    own_grad = pltpu.make_async_copy(grad_in, grad_slots.at[col], own_sem.at[1])
    own_tok.start()
    own_grad.start()
    pl.semaphore_wait(barrier, rows - 1 + cols - 1)

    def gather(s, slot):
        to = (row, (col + s) % cols)
        return [
            pltpu.make_async_remote_copy(
                src_ref=src, dst_ref=dst.at[slot], send_sem=tok_ssem.at[a, s], recv_sem=tok_rsem.at[a, s],
                device_id=to, device_id_type=MESH,
            )
            for a, (src, dst) in enumerate(((tok_in, tok_slots), (grad_in, grad_slots)))
        ]

    for s in range(1, cols):
        for copy in gather(s, col):
            copy.start()
    for trio in loads[1:]:
        for load in trio:
            load.start()
    own_tok.wait()
    own_grad.wait()
    for s in range(1, cols):
        for copy in gather(s, (col + cols - s) % cols):
            copy.wait_recv()
    for slots, whole in ((tok_slots, tok_all), (grad_slots, grad_all)):
        for k in range(cols):
            stage[k * few : (k + 1) * few, :] = slots[k].astype(F32)
        whole[...] = stage[...].astype(BF16)
    outs = [
        pltpu.make_async_copy(tok_all, tok_out, out_sem.at[0]),
        pltpu.make_async_copy(grad_all, grad_out, out_sem.at[1]),
    ]
    for copy in outs:
        copy.start()

    def partial(o):
        for load in loads[o]:
            load.wait()
        gate_part = jnp.dot(tok_all[...], gate_buf[o], preferred_element_type=F32)
        up_part = jnp.dot(tok_all[...], up_buf[o], preferred_element_type=F32)
        back_part = lax.dot_general(down_buf[o], grad_all[...], LAST, preferred_element_type=F32).T
        return gate_part, up_part, back_part

    sends = []
    for o, (dy, dc) in enumerate(offsets[:-1]):
        for i, part in enumerate(partial(o)):
            part_send[o, i] = part.astype(BF16)
        copy = pltpu.make_async_remote_copy(
            src_ref=part_send.at[o], dst_ref=part_recv.at[o],
            send_sem=part_ssem.at[o], recv_sem=part_rsem.at[o],
            device_id=(peer(dy, dc), col), device_id_type=MESH,
        )
        copy.start()
        sends.append(copy)
    last = rows - 1
    sums = list(partial(last))
    for o in range(rows - 1):
        sends[o].wait_recv()
        sums = [total + part_recv[o, i].astype(F32) for i, total in enumerate(sums)]
    for i, value in enumerate(hidden_grads(*sums)):
        acts[row, i] = value

    def share(sems, n, q, to):
        return pltpu.make_async_remote_copy(
            src_ref=acts.at[q], dst_ref=acts.at[q], send_sem=sems[0].at[n], recv_sem=sems[1].at[n],
            device_id=(to, col), device_id_type=MESH,
        )

    direct, forward = (acts_ssem, acts_rsem), (fwd_ssem, fwd_rsem)
    other = peer(0, 1)
    for dy in range(1, chips):
        share(direct, dy, row, peer(dy, 0)).start()
    share(forward, 0, row, other).start()

    block = acc.shape[0] // 4

    def add_block(o, q, first):
        @pl.loop(0, 4)
        def _(t):
            at = pl.ds(pl.multiple_of(t * block, block), block)
            value = lax.dot_general(gate_buf[o, at, :], acts[q, 1], LAST, preferred_element_type=F32)
            value += lax.dot_general(up_buf[o, at, :], acts[q, 2], LAST, preferred_element_type=F32)
            acc[at, :] = value if first else acc[at, :] + value

    add_block(last, row, True)
    share(forward, 0, other, other).wait_recv()
    add_block(last - 1, other, False)
    for dy in range(1, chips):
        q = peer(chips - dy, 0)
        share(direct, dy, q, peer(dy, 0)).wait_recv()
        share(forward, dy, q, other).start()
        add_block(2 * (chips - dy - 1), q, False)
    for dy in range(1, chips):
        q = peer(chips - dy, 1)
        share(forward, dy, q, other).wait_recv()
        add_block(2 * (chips - dy - 1) + 1, q, False)

    total = acc[...].T
    stage[...] = total
    for k in range(cols):
        dtok_send[k] = stage[k * few : (k + 1) * few, :].astype(BF16)

    def scatter(s):
        to = (col + s) % cols
        return pltpu.make_async_remote_copy(
            src_ref=dtok_send.at[to], dst_ref=dtok_recv.at[s], send_sem=dtok_ssem.at[s],
            recv_sem=dtok_rsem.at[s], device_id=(row, to), device_id_type=MESH,
        )

    for s in range(1, cols):
        scatter(s).start()
    outs.append(pltpu.make_async_copy(acts, acts_out, out_sem.at[2]))
    outs[-1].start()
    result = dtok_send[col].astype(F32)
    for s in range(1, cols):
        scatter(s).wait_recv()
        result += dtok_recv[s].astype(F32)
    dtok_out[...] = result.astype(BF16)

    for copy in outs:
        copy.wait()
    for s in range(1, cols):
        for copy in gather(s, col):
            copy.wait_send()
        scatter(s).wait_send()
    for copy in sends:
        copy.wait_send()
    share(forward, 0, row, other).wait_send()
    for dy in range(1, chips):
        share(direct, dy, row, peer(dy, 0)).wait_send()
        share(forward, dy, peer(chips - dy, 0), other).wait_send()


def exchange(rows, cols, tokens, grad_out, gate_weight, up_weight, down_weight):
    few, depth = tokens.shape
    hidden = gate_weight.shape[1]
    width = hidden // rows
    many = few * cols
    dma = pltpu.SemaphoreType.DMA
    any_spec = pl.BlockSpec(memory_space=pl.ANY)
    vmem_spec = pl.BlockSpec(memory_space=pltpu.VMEM)
    shape = jax.ShapeDtypeStruct
    return pl.pallas_call(
        functools.partial(exchange_kernel, rows, cols),
        out_shape=(
            shape((many, depth), BF16),
            shape((many, depth), BF16),
            shape((rows, 3, many, width), BF16),
            shape((few, depth), BF16),
        ),
        in_specs=[vmem_spec, vmem_spec, any_spec, any_spec, any_spec],
        out_specs=(any_spec, any_spec, any_spec, vmem_spec),
        scratch_shapes=[
            pltpu.VMEM((rows, depth, width), BF16),
            pltpu.VMEM((rows, depth, width), BF16),
            pltpu.VMEM((rows, width, depth), BF16),
            pltpu.VMEM((cols, few, depth), BF16),
            pltpu.VMEM((cols, few, depth), BF16),
            pltpu.VMEM((many, depth), F32),
            pltpu.VMEM((many, depth), BF16),
            pltpu.VMEM((many, depth), BF16),
            pltpu.VMEM((rows - 1, 3, many, width), BF16),
            pltpu.VMEM((rows - 1, 3, many, width), BF16),
            pltpu.VMEM((rows, 3, many, width), BF16),
            pltpu.VMEM((depth, many), F32),
            pltpu.VMEM((cols, few, depth), BF16),
            pltpu.VMEM((cols, few, depth), BF16),
            dma((3, rows)),
            dma((2,)),
            dma((2, cols)),
            dma((2, cols)),
            dma((rows,)),
            dma((rows,)),
            dma((rows,)),
            dma((rows,)),
            dma((rows,)),
            dma((rows,)),
            dma((cols,)),
            dma((cols,)),
            dma((3,)),
        ],
        compiler_params=pltpu.CompilerParams(
            collective_id=0, has_side_effects=True, vmem_limit_bytes=62 * 1024 * 1024
        ),
        name="exchange",
    )(tokens, grad_out, gate_weight, up_weight, down_weight)


def outer_kernel(tok, grad, acts, gate_out, up_out, down_out, hidden_t):
    rows, _, _, width = acts.shape

    @pl.when(pl.program_id(0) == 0)
    def _():
        for q in range(rows):
            hidden_t[q * width : (q + 1) * width, :] = acts[q, 0].astype(F32).T.astype(BF16)

    tok_t = tok[...].astype(F32).T.astype(BF16)
    for out, i in ((gate_out, 1), (up_out, 2)):
        @pl.loop(0, rows)
        def _(q):
            at = pl.ds(pl.multiple_of(q * width, 128), width)
            out[:, at] = jnp.dot(tok_t, acts[q, i], preferred_element_type=F32).astype(BF16)

    @pl.loop(0, 2 * rows)
    def _(t):
        at = pl.ds(pl.multiple_of(t * (width // 2), 64), width // 2)
        down_out[at, :] = jnp.dot(hidden_t[at, :], grad[...], preferred_element_type=F32).astype(BF16)


def outer(tok, grad, acts):
    many, depth = tok.shape
    rows, _, _, width = acts.shape
    hidden = rows * width
    steps = 8
    while depth % (steps * 128):
        steps //= 2
    part = depth // steps
    shape = jax.ShapeDtypeStruct
    return pl.pallas_call(
        outer_kernel,
        grid=(steps,),
        out_shape=(
            shape((depth, hidden), BF16),
            shape((depth, hidden), BF16),
            shape((hidden, depth), BF16),
        ),
        in_specs=[
            pl.BlockSpec((many, part), lambda i: (0, i)),
            pl.BlockSpec((many, part), lambda i: (0, i)),
            pl.BlockSpec((rows, 3, many, width), lambda i: (0, 0, 0, 0)),
        ],
        out_specs=(
            pl.BlockSpec((part, hidden), lambda i: (i, 0)),
            pl.BlockSpec((part, hidden), lambda i: (i, 0)),
            pl.BlockSpec((hidden, part), lambda i: (0, i)),
        ),
        scratch_shapes=[pltpu.VMEM((hidden, many), BF16)],
        compiler_params=pltpu.CompilerParams(
            dimension_semantics=("arbitrary",), vmem_limit_bytes=40 * 1024 * 1024
        ),
        name="outer",
    )(tok, grad, acts)


def shards(rows, cols, tokens, grad_out, gate_weight, up_weight, down_weight):
    tok, grad, acts, grad_tokens = exchange(
        rows, cols, tokens, grad_out, gate_weight, up_weight, down_weight
    )
    return (grad_tokens, *outer(tok, grad, acts))


def plain_shards(tokens, grad_out, gate_weight, up_weight, down_weight):
    tok_full, grad_full = (
        lax.all_gather(tokens, "col", axis=0, tiled=True),
        lax.all_gather(grad_out, "col", axis=0, tiled=True),
    )
    hidden_width = gate_weight.shape[1]
    gate_part = jnp.dot(tok_full, gate_weight, preferred_element_type=F32)
    up_part = jnp.dot(tok_full, up_weight, preferred_element_type=F32)
    back_part = jnp.einsum("td,fd->tf", grad_full, down_weight, preferred_element_type=F32)
    sums = lax.psum(jnp.concatenate([gate_part, up_part, back_part], axis=1), "row")
    hidden, grad_gate, grad_up = hidden_grads(*jnp.split(sums, 3, axis=1))
    grad_down_weight = jnp.einsum("tf,td->fd", hidden, grad_full, preferred_element_type=F32).astype(BF16)
    grad_gate_weight = jnp.einsum("td,tf->df", tok_full, grad_gate, preferred_element_type=F32).astype(BF16)
    grad_up_weight = jnp.einsum("td,tf->df", tok_full, grad_up, preferred_element_type=F32).astype(BF16)
    total = jnp.einsum("tf,df->td", grad_gate, gate_weight, preferred_element_type=F32)
    total += jnp.einsum("tf,df->td", grad_up, up_weight, preferred_element_type=F32)
    grad_tokens = lax.psum_scatter(total, "col", scatter_dimension=0, tiled=True).astype(BF16)
    return (grad_tokens, grad_gate_weight, grad_up_weight, grad_down_weight)


def choose(rows, cols, *operands):
    depth, hidden = operands[2].shape
    if hidden % (rows * 128) or depth % 128 or rows % 2:
        return plain_shards(*operands)
    return shards(rows, cols, *operands)


def solution(mesh):
    placed = (P("col", "row"), P("col", "row"), P("row", "col"), P("row", "col"), P("col", "row"))
    return jax.shard_map(
        functools.partial(choose, mesh.shape["row"], mesh.shape["col"]),
        mesh=mesh,
        in_specs=placed,
        out_specs=(P("col", "row"), P("row", "col"), P("row", "col"), P("col", "row")),
        check_vma=False,
    )
```
